32 devices in a mesh: rep: 2 (over y), shard: 16 (over z, x, core).
Axes of the slice: x: 2, y: 2, z: 4, core: 2. Of those that a mesh axis runs over, the one named last changes fastest.
Arguments:
- activations: bfloat16 [32768, 2048], P(('rep', 'shard')), may hold values from -6 to 6
- cotangents: bfloat16 [32768, 1024], P(('rep', 'shard')), may hold values from -768 to 768
- inner_params: float32 [2, 2048, 1024], P('rep', 'shard'), may hold values from -6 to 6
- inner_moment: float32 [2, 2048, 1024], P('rep', 'shard'), may hold values from 0.25 to 4
- outer_params: float32 [2048, 1024], P('shard'), may hold values from -6 to 6
- momentum: float32 [2048, 1024], P('shard'), may hold values from -3 to 3
Outputs:
- new_params: float32 [2048, 1024], P('shard')
- new_momentum: float32 [2048, 1024], P('shard')
- compute_copy: bfloat16 [2048, 1024], replicated
The draws below stay inside these ranges and needn't reach their ends.
All inputs are finite; a program needn't handle non-finite values.
Results may differ from the reference program's by a relative error of at most 0.007.
Values may be sent and summed in bfloat16 or wider, within the bound.
A program may use at most 64 MiB of HBM per device.

```python
import math
import jax
import jax.numpy as jnp
from jax import lax

D = 2048
KV = 1024
TOK_DEV = 1024
REPS = 2
GROUP_TOK = 16384
TOKENS = 32768
N_SHARD = 16


def with_spikes(drawn, own_key, source, target, blocks, factor):
    def block_of(axis_at):
        return (jnp.arange(drawn.shape[axis_at]) // (drawn.shape[axis_at] // blocks)).reshape((-1,) + (1,) * (drawn.ndim - 1 - axis_at))

    first = jax.random.permutation(own_key, blocks)[block_of(target)]
    other_side = (block_of(target) + blocks // 2) % blocks
    return jnp.where((block_of(source) == first) | (block_of(source) == other_side), factor * drawn, drawn)


def shard_levels(stream_key, extent, pieces, least, top_value):
    gain, own = 1.0, jax.random.fold_in(stream_key, 6)
    for position, blocks in pieces:
        heights = jnp.exp(jax.random.uniform(jax.random.fold_in(own, position), (blocks,), jnp.float32, least / len(pieces), top_value / len(pieces)))
        gain = gain * jnp.repeat(heights, extent[position] // blocks).reshape([-1 if axis == position else 1 for axis in range(len(extent))])
    return gain


def bell_draw(stream_key, dims, width, bound, cuts=(), held_as=jnp.bfloat16):
    result = jax.random.normal(stream_key, dims, jnp.float32) * width
    if len(cuts) > 0:
        result = shard_levels(stream_key, dims, cuts, -0.22, 0.18) * result
    return jnp.clip(result, min=-bound, max=bound).astype(held_as)


def noise_with(own_key, dims, spread, reach, pieces, heavy, held_as=jnp.bfloat16):
    array = spread * jax.random.normal(own_key, dims, jnp.float32)
    if pieces:
        array = array * shard_levels(own_key, dims, pieces, -0.22, 0.18)
    return jnp.clip(with_spikes(array, jax.random.fold_in(own_key, 3), *heavy), -reach, reach).astype(held_as)


def setup_inputs(seed: int = 0) -> dict:
    seeds = jax.random.split(jax.random.key(seed), 7)
    activations = noise_with(seeds[0], (TOKENS, D), 1.0, 6.0, ((0, 32),), (0, 1, 32, 2.75))
    cotangents = bell_draw(seeds[1], (TOKENS, KV), (GROUP_TOK ** 0.5), 768.0, ((0, 32),))
    inner_params = bell_draw(seeds[2], (REPS, D, KV), 1.0, 6.0, ((0, 2), (1, 16)), jnp.float32)
    inner_moment = jnp.clip(jnp.exp(math.log(4.0) - 2.7725887 * jax.random.uniform(seeds[3], (REPS, D, KV), jnp.float32) ** shard_levels(seeds[3], (REPS, D, KV), ((0, 2), (1, 16)), -0.2, 0.2)), 0.25, 4.0)
    outer_params = bell_draw(seeds[4], (D, KV), 1.0, 6.0, ((0, 16),), jnp.float32)
    momentum = bell_draw(seeds[5], (D, KV), 0.5, 3.0, ((0, 16),), jnp.float32)
    return dict(activations=activations, cotangents=cotangents, inner_params=inner_params, inner_moment=inner_moment, outer_params=outer_params, momentum=momentum)


outer_rate = 0.7
inertia = 0.9
inner_rate = 0.3
epsilon = 1e-08

def reference(activations, cotangents, inner_params, inner_moment, outer_params, momentum):
    group_tok = TOK_DEV * N_SHARD
    delta_total = jnp.zeros(outer_params.shape, jnp.float32)
    for replica in range(REPS):
        rows_act = activations[replica * group_tok:(replica + 1) * group_tok]
        rows_cot = cotangents[replica * group_tok:(replica + 1) * group_tok]
        summed = lax.dot_general(rows_act, rows_cot, (((0,), (0,)), ((), ())), preferred_element_type=jnp.float32)
        mean_grad = summed / group_tok
        replica_params = inner_params[replica] - inner_rate * mean_grad / (jnp.sqrt(inner_moment[replica]) + epsilon)
        delta_total = delta_total + (outer_params - replica_params)
    pseudo_grad = delta_total / REPS
    new_momentum = inertia * momentum + pseudo_grad
    new_params = outer_params - outer_rate * (pseudo_grad + inertia * new_momentum)
    return (new_params, new_momentum, new_params.astype(jnp.bfloat16))
```

```python
import functools

import jax
import jax.numpy as jnp
from jax import lax
from jax.experimental import pallas as pl
from jax.experimental.pallas import tpu as pltpu
from jax.sharding import PartitionSpec as P

outer_rate = 0.7
inertia = 0.9
inner_rate = 0.3
epsilon = 1e-08

CORES = 2
MESH = pl.DeviceIdType.MESH


def kernel(
    reps, deep, wide, chunks, group_tok,
    act, cot, inner, moment, outer, mom,
    new_params, new_moment, copy_out,
    act_t, own, pair_out, pair_in, x_out, x_in, z_out, z_in, deltas, gathered,
    pair_s, pair_r, x_s, x_r, z_s, z_r, y_s, y_r,
    gz_s, gz_r, gx_s, gx_r, gy_s, gy_r, gp_s, gp_r, out_s,
):
    rep = lax.axis_index("rep")
    shard = lax.axis_index("shard")
    core = lax.rem(shard, CORES)
    x = lax.rem(shard // CORES, wide)
    z = shard // (CORES * wide)
    rows = inner.shape[1]
    width = own.shape[-1]
    blocks = deep * wide

    def place(zz, xx, cc):
        return (zz * wide + xx) * CORES + cc

    def z_at(step):
        return lax.rem(z + step, deep)

    def x_at(step):
        return lax.rem(x + step, wide)

    def rep_at(step):
        return lax.rem(rep + step, reps)

    partner = (rep, place(z, x, 1 - core))
    x_peers = [(rep, place(z, x_at(d), core)) for d in range(1, wide)]
    z_peers = [(rep, place(z_at(d), x, core)) for d in range(1, deep)]
    y_peers = [(rep_at(d), shard) for d in range(1, reps)]
    peers = [partner] + x_peers + z_peers + y_peers

    def send(src, dst, s, r, device):
        return pltpu.make_async_remote_copy(
            src_ref=src, dst_ref=dst, send_sem=s, recv_sem=r, device_id=device, device_id_type=MESH
        )

    barrier = pltpu.get_barrier_semaphore()
    for peer in peers:
        pl.semaphore_signal(barrier, inc=1, device_id=peer, device_id_type=MESH)

    def pair_copy(k):
        return send(pair_out.at[k], pair_in.at[k], pair_s.at[k], pair_r.at[k], partner)

    def x_copies(k):
        return [
            send(x_out.at[k, d], x_in.at[k, d], x_s.at[k, d], x_r.at[k, d], peer)
            for d, peer in enumerate(x_peers)
        ]

    def z_copies(k):
        return [
            send(z_out.at[k, d], z_in.at[k, d], z_s.at[k, d], z_r.at[k, d], peer)
            for d, peer in enumerate(z_peers)
        ]

    def y_copies(k):
        return [
            send(deltas.at[k, rep], deltas.at[k, rep], y_s.at[k, d], y_r.at[k, d], peer)
            for d, peer in enumerate(y_peers)
        ]

    def part(k, piece):
        if piece < deep:
            return gathered.at[k, z_at(piece), x, core]
        return gathered.at[k, :, x_at(piece - deep + 1), core]

    pieces = deep + wide - 1

    def gz_copies(k):
        return [
            send(part(k, 0), part(k, 0), gz_s.at[k, d], gz_r.at[k, d], peer)
            for d, peer in enumerate(z_peers)
        ]

    def gx_copies(k):
        column = gathered.at[k, :, x, core]
        return [
            send(column, column, gx_s.at[k, d], gx_r.at[k, d], peer)
            for d, peer in enumerate(x_peers)
        ]

    def gy_copies(k, piece):
        return [
            send(part(k, piece), part(k, piece), gy_s.at[k, piece, d], gy_r.at[k, piece, d], peer)
            for d, peer in enumerate(y_peers)
        ]

    def gp_copy(k, piece):
        return send(
            part(k, piece), part(k, piece), gp_s.at[k, piece], gp_r.at[k, piece], partner
        )

    def out_copy(k):
        return pltpu.make_async_copy(
            gathered.at[k], copy_out.at[:, :, :, :, pl.ds(k * width, width)], out_s.at[k]
        )

    def start(copies):
        for c in copies:
            c.start()

    def arrived(copies):
        for c in copies:
            c.wait_recv()

    def sent(copies):
        for c in copies:
            c.wait_send()

    def on_plane(k, here, elsewhere=None):
        pl.when(rep == k % reps)(here)
        if elsewhere is not None:
            pl.when(rep != k % reps)(elsewhere)

    group = 2 if chunks % 2 == 0 else 1
    span = group * width

    def product(side, m):
        return lax.dot_general(
            act_t[:, side].reshape(blocks * rows, act.shape[0]),
            cot[:, m * span:(m + 1) * span],
            (((1,), (0,)), ((), ())),
            preferred_element_type=jnp.float32,
        )

    def theirs(m):
        value = product(1 - core, m).astype(jnp.bfloat16)
        for i in range(group):
            pair_out[m * group + i] = value[:, i * width:(i + 1) * width].reshape(
                deep, wide, rows, width
            )
        if m == 0:
            pl.semaphore_wait(barrier, len(peers))
        for i in range(group):
            pair_copy(m * group + i).start()

    def ours(m):
        value = product(core, m)
        for i in range(group):
            own[m * group + i] = value[:, i * width:(i + 1) * width].reshape(
                deep, wide, rows, width
            )

    def to_x(k):
        pair_copy(k).wait_recv()
        for d in range(1, wide):
            xx = x_at(d)
            x_out[k, d - 1] = (own[k, :, xx] + pair_in[k, :, xx].astype(jnp.float32)).astype(
                jnp.bfloat16
            )
        start(x_copies(k))

    def layer_sum(k, zz):
        total = own[k, zz, x] + pair_in[k, zz, x].astype(jnp.float32)
        for d in range(wide - 1):
            total = total + x_in[k, d, zz].astype(jnp.float32)
        return total

    def to_z(k):
        arrived(x_copies(k))
        for d in range(1, deep):
            z_out[k, d - 1] = layer_sum(k, z_at(d)).astype(jnp.bfloat16)
        start(z_copies(k))

    def to_y(k):
        cols = slice(k * width, (k + 1) * width)
        total = layer_sum(k, z)
        arrived(z_copies(k))
        for d in range(deep - 1):
            total = total + z_in[k, d].astype(jnp.float32)
        mean_grad = total / group_tok
        replica = inner[0, :, cols] - inner_rate * mean_grad / (
            jnp.sqrt(moment[0, :, cols]) + epsilon
        )
        deltas[k, rep] = outer[:, cols] - replica
        start(y_copies(k))

    def update(k):
        cols = slice(k * width, (k + 1) * width)
        arrived(y_copies(k))
        total = deltas[k, 0]
        for r in range(1, reps):
            total = total + deltas[k, r]
        pseudo = total / reps
        fresh_moment = inertia * mom[:, cols] + pseudo
        fresh = outer[:, cols] - outer_rate * (pseudo + inertia * fresh_moment)
        new_params[:, cols] = fresh
        new_moment[:, cols] = fresh_moment
        gathered[k, z, x, core] = fresh.astype(jnp.bfloat16)

        def here():
            start(gz_copies(k))

        on_plane(k, here)
        gp_copy(k, 0).start()

    def column_in(k):
        def here():
            arrived(gz_copies(k))
            start(gx_copies(k))
            for piece in range(1, deep):
                start(gy_copies(k, piece))
                gp_copy(k, piece).start()

        on_plane(k, here)

    def pieces_in(k):
        def here():
            arrived(gx_copies(k))
            for piece in range(deep, pieces):
                start(gy_copies(k, piece))
                gp_copy(k, piece).start()

        def elsewhere():
            step = lax.rem(rep + reps - k % reps, reps)
            for piece in range(1, pieces):
                landed(k, piece, step).wait_recv()
                gp_copy(k, piece).start()

        on_plane(k, here, elsewhere)

    def landed(k, piece, step):
        return send(
            part(k, piece), part(k, piece), gy_s.at[k, piece, step - 1],
            gy_r.at[k, piece, step - 1], y_peers[0],
        )

    def finish(k):
        for piece in range(pieces):
            gp_copy(k, piece).wait_recv()
        out_copy(k).start()

    def drain(k):
        pair_copy(k).wait_send()
        sent(x_copies(k) + z_copies(k) + y_copies(k))

        def here():
            sent(gz_copies(k) + gx_copies(k))
            for piece in range(1, pieces):
                sent(gy_copies(k, piece))

        on_plane(k, here)
        for piece in range(pieces):
            gp_copy(k, piece).wait_send()
        out_copy(k).wait()

    for j in range(blocks):
        strip = act[:, j * CORES * rows:(j + 1) * CORES * rows]
        act_t[j] = strip.T.reshape(CORES, rows, act.shape[0])

    products = chunks // group
    theirs(0)
    ours(0)
    for m in range(products):
        if m + 1 < products:
            theirs(m + 1)
        for i in range(group):
            to_x(m * group + i)
        if m + 1 < products:
            ours(m + 1)
    stages = ((to_z, 0), (to_y, 2), (update, 3), (column_in, 5), (pieces_in, 6), (finish, 8))
    for tick in range(chunks + stages[-1][1]):
        for stage, lag in stages:
            if 0 <= tick - lag < chunks:
                stage(tick - lag)
    for k in range(chunks):
        drain(k)


def per_device(deep, wide, activations, cotangents, inner_params, inner_moment, outer_params, momentum):
    reps = lax.axis_size("rep")
    shards = lax.axis_size("shard")
    tokens, model = activations.shape
    kv = cotangents.shape[1]
    rows = outer_params.shape[0]
    width = 128
    chunks = kv // width
    bf16, f32 = jnp.bfloat16, jnp.float32
    tile = (rows, width)
    vmem = pl.BlockSpec(memory_space=pltpu.VMEM)
    dma = pltpu.SemaphoreType.DMA
    pieces = deep + wide - 1
    new_params, new_momentum, copied = pl.pallas_call(
        functools.partial(kernel, reps, deep, wide, chunks, tokens * shards),
        out_shape=(
            jax.ShapeDtypeStruct((rows, kv), f32),
            jax.ShapeDtypeStruct((rows, kv), f32),
            jax.ShapeDtypeStruct((deep, wide, CORES, rows, kv), bf16),
        ),
        in_specs=[vmem] * 6,
        out_specs=(vmem, vmem, pl.BlockSpec(memory_space=pl.ANY)),
        scratch_shapes=[
            pltpu.VMEM((deep * wide, CORES, rows, tokens), bf16),
            pltpu.VMEM((chunks, deep, wide) + tile, f32),
            pltpu.VMEM((chunks, deep, wide) + tile, bf16),
            pltpu.VMEM((chunks, deep, wide) + tile, bf16),
            pltpu.VMEM((chunks, wide - 1, deep) + tile, bf16),
            pltpu.VMEM((chunks, wide - 1, deep) + tile, bf16),
            pltpu.VMEM((chunks, deep - 1) + tile, bf16),
            pltpu.VMEM((chunks, deep - 1) + tile, bf16),
            pltpu.VMEM((chunks, reps) + tile, f32),
            pltpu.VMEM((chunks, deep, wide, CORES) + tile, bf16),
            dma((chunks,)), dma((chunks,)),
            dma((chunks, wide - 1)), dma((chunks, wide - 1)),
            dma((chunks, deep - 1)), dma((chunks, deep - 1)),
            dma((chunks, reps - 1)), dma((chunks, reps - 1)),
            dma((chunks, deep - 1)), dma((chunks, deep - 1)),
            dma((chunks, wide - 1)), dma((chunks, wide - 1)),
            dma((chunks, pieces, reps - 1)), dma((chunks, pieces, reps - 1)),
            dma((chunks, pieces)), dma((chunks, pieces)),
            dma((chunks,)),
        ],
        compiler_params=pltpu.CompilerParams(
            collective_id=0, has_side_effects=True, vmem_limit_bytes=58 * 1024 * 1024
        ),
    )(activations, cotangents, inner_params, inner_moment, outer_params, momentum)
    return (new_params, new_momentum, copied.reshape(model, kv))


def layout(mesh):
    chips = mesh.shape["shard"] // CORES
    first = mesh.devices.reshape(mesh.shape["rep"], mesh.shape["shard"])[0]
    wide = len({d.coords[0] for d in first}) if hasattr(first[0], "coords") else 2
    return chips // wide, wide


def solution(mesh):
    deep, wide = layout(mesh)
    in_specs = (
        P(("rep", "shard"), None),
        P(("rep", "shard"), None),
        P("rep", "shard", None),
        P("rep", "shard", None),
        P("shard", None),
        P("shard", None),
    )
    out_specs = (P("shard", None), P("shard", None), P())
    return jax.shard_map(
        functools.partial(per_device, deep, wide),
        mesh=mesh, in_specs=in_specs, out_specs=out_specs, check_vma=False,
    )
```

```python
import functools

import jax
import jax.numpy as jnp
from jax import lax
from jax.experimental import pallas as pl
from jax.experimental.pallas import tpu as pltpu
from jax.sharding import PartitionSpec as P

outer_rate = 0.7
inertia = 0.9
inner_rate = 0.3
epsilon = 1e-08

CORES = 2
MESH = pl.DeviceIdType.MESH


def kernel(
    reps, deep, wide, chunks, group_tok,
    act_in, cot_in, inner_in, moment_in, outer_in, mom_in,
    new_params, new_moment, copy_out,
    act, cot, inner, moment, outer, mom,
    act_t, own, pair_out, pair_in, x_out, x_in, z_out, z_in, deltas, gathered,
    pair_s, pair_r, x_s, x_r, z_s, z_r, y_s, y_r,
    gz_s, gz_r, gx_s, gx_r, gy_s, gy_r, gp_s, gp_r, load_s,
):
    rep = lax.axis_index("rep")
    shard = lax.axis_index("shard")
    core = lax.rem(shard, CORES)
    x = lax.rem(shard // CORES, wide)
    z = shard // (CORES * wide)
    rows = inner.shape[1]
    loads = [
        pltpu.make_async_copy(src, dst, load_s.at[i])
        for i, (src, dst) in enumerate((
            (act_in, act), (cot_in, cot), (inner_in, inner), (moment_in, moment),
            (outer_in, outer), (mom_in, mom),
        ))
    ]
    for load in loads:
        load.start()
    width = own.shape[-1]
    blocks = deep * wide

    def place(zz, xx, cc):
        return (zz * wide + xx) * CORES + cc

    def z_at(step):
        return lax.rem(z + step, deep)

    def x_at(step):
        return lax.rem(x + step, wide)

    def rep_at(step):
        return lax.rem(rep + step, reps)

    partner = (rep, place(z, x, 1 - core))
    x_peers = [(rep, place(z, x_at(d), core)) for d in range(1, wide)]
    z_peers = [(rep, place(z_at(d), x, core)) for d in range(1, deep)]
    y_peers = [(rep_at(d), shard) for d in range(1, reps)]
    peers = [partner] + x_peers + z_peers + y_peers

    def send(src, dst, s, r, device):
        return pltpu.make_async_remote_copy(
            src_ref=src, dst_ref=dst, send_sem=s, recv_sem=r, device_id=device, device_id_type=MESH
        )

    barrier = pltpu.get_barrier_semaphore()
    for peer in peers:
        pl.semaphore_signal(barrier, inc=1, device_id=peer, device_id_type=MESH)

    def pair_copy(k):
        return send(pair_out.at[k], pair_in.at[k], pair_s.at[k], pair_r.at[k], partner)

    def x_copies(k):
        return [
            send(x_out.at[k, d], x_in.at[k, d], x_s.at[k, d], x_r.at[k, d], peer)
            for d, peer in enumerate(x_peers)
        ]

    def z_copies(k):
        return [
            send(z_out.at[k, d], z_in.at[k, d], z_s.at[k, d], z_r.at[k, d], peer)
            for d, peer in enumerate(z_peers)
        ]

    def y_copies(k):
        return [
            send(deltas.at[k, rep], deltas.at[k, rep], y_s.at[k, d], y_r.at[k, d], peer)
            for d, peer in enumerate(y_peers)
        ]

    def part(k, piece):
        if piece < deep:
            return gathered.at[k, z_at(piece), x, core]
        return gathered.at[k, :, x_at(piece - deep + 1), core]

    pieces = deep + wide - 1

    def gz_copies(k):
        return [
            send(part(k, 0), part(k, 0), gz_s.at[k, d], gz_r.at[k, d], peer)
            for d, peer in enumerate(z_peers)
        ]

    def gx_copies(k):
        column = gathered.at[k, :, x, core]
        return [
            send(column, column, gx_s.at[k, d], gx_r.at[k, d], peer)
            for d, peer in enumerate(x_peers)
        ]

    def gy_copies(k, piece):
        return [
            send(part(k, piece), part(k, piece), gy_s.at[k, piece, d], gy_r.at[k, piece, d], peer)
            for d, peer in enumerate(y_peers)
        ]

    def gp_copy(k, piece):
        return send(
            part(k, piece), part(k, piece), gp_s.at[k, piece], gp_r.at[k, piece], partner
        )

    def start(copies):
        for c in copies:
            c.start()

    def arrived(copies):
        for c in copies:
            c.wait_recv()

    def sent(copies):
        for c in copies:
            c.wait_send()

    def on_plane(k, here):
        pl.when(rep == k % reps)(here)

    group = 2 if chunks % 2 == 0 else 1
    span = group * width

    def product(side, m):
        return lax.dot_general(
            act_t[:, side].reshape(blocks * rows, act.shape[0]),
            cot[:, m * span:(m + 1) * span],
            (((1,), (0,)), ((), ())),
            preferred_element_type=jnp.float32,
        )

    def theirs(m):
        value = product(1 - core, m).astype(jnp.bfloat16)
        for i in range(group):
            pair_out[m * group + i] = value[:, i * width:(i + 1) * width].reshape(
                deep, wide, rows, width
            )
        if m == 0:
            pl.semaphore_wait(barrier, len(peers))
        for i in range(group):
            pair_copy(m * group + i).start()

    def ours(m):
        value = product(core, m)
        for i in range(group):
            own[m * group + i] = value[:, i * width:(i + 1) * width].reshape(
                deep, wide, rows, width
            )

    def to_x(k):
        pair_copy(k).wait_recv()
        for d in range(1, wide):
            xx = x_at(d)
            x_out[k, d - 1] = (own[k, :, xx] + pair_in[k, :, xx].astype(jnp.float32)).astype(
                jnp.bfloat16
            )
        start(x_copies(k))

    def layer_sum(k, zz):
        total = own[k, zz, x] + pair_in[k, zz, x].astype(jnp.float32)
        for d in range(wide - 1):
            total = total + x_in[k, d, zz].astype(jnp.float32)
        return total

    def to_z(k):
        arrived(x_copies(k))
        for d in range(1, deep):
            z_out[k, d - 1] = layer_sum(k, z_at(d)).astype(jnp.bfloat16)
        start(z_copies(k))

    def to_y(k):
        cols = slice(k * width, (k + 1) * width)
        total = layer_sum(k, z)
        arrived(z_copies(k))
        for d in range(deep - 1):
            total = total + z_in[k, d].astype(jnp.float32)
        mean_grad = total / group_tok
        replica = inner[0, :, cols] - inner_rate * mean_grad / (
            jnp.sqrt(moment[0, :, cols]) + epsilon
        )
        deltas[k, rep] = outer[:, cols] - replica
        start(y_copies(k))

    def update(k):
        cols = slice(k * width, (k + 1) * width)
        arrived(y_copies(k))
        total = deltas[k, 0]
        for r in range(1, reps):
            total = total + deltas[k, r]
        pseudo = total / reps
        fresh_moment = inertia * mom[:, cols] + pseudo
        fresh = outer[:, cols] - outer_rate * (pseudo + inertia * fresh_moment)
        new_params[:, cols] = fresh
        new_moment[:, cols] = fresh_moment
        gathered[k, z, x, core] = fresh.astype(jnp.bfloat16)

        def here():
            start(gz_copies(k))

        on_plane(k, here)
        gp_copy(k, 0).start()

    def column_in(k):
        def here():
            arrived(gz_copies(k))
            start(gx_copies(k))
            for piece in range(1, deep):
                start(gy_copies(k, piece))
                gp_copy(k, piece).start()

        on_plane(k, here)

    def pieces_in(k):
        def here():
            arrived(gx_copies(k))
            for piece in range(deep, pieces):
                start(gy_copies(k, piece))
                gp_copy(k, piece).start()

        on_plane(k, here)

    def from_y(k):
        def elsewhere():
            step = lax.rem(rep + reps - k % reps, reps)
            for piece in range(1, pieces):
                landed(k, piece, step).wait_recv()
                gp_copy(k, piece).start()

        pl.when(rep != k % reps)(elsewhere)

    def landed(k, piece, step):
        return send(
            part(k, piece), part(k, piece), gy_s.at[k, piece, step - 1],
            gy_r.at[k, piece, step - 1], y_peers[0],
        )

    def finish(k):
        for piece in range(pieces):
            gp_copy(k, piece).wait_recv()
        copy_out[:, :, :, :, k * width:(k + 1) * width] = gathered[k]

    def drain(k):
        pair_copy(k).wait_send()
        sent(x_copies(k) + z_copies(k) + y_copies(k))

        def here():
            sent(gz_copies(k) + gx_copies(k))
            for piece in range(1, pieces):
                sent(gy_copies(k, piece))

        on_plane(k, here)
        for piece in range(pieces):
            gp_copy(k, piece).wait_send()

    loads[0].wait()
    for j in range(blocks):
        strip = act[:, j * CORES * rows:(j + 1) * CORES * rows]
        act_t[j] = strip.T.reshape(CORES, rows, act.shape[0])

    products = chunks // group
    loads[1].wait()
    theirs(0)
    ours(0)
    for m in range(products):
        if m + 1 < products:
            theirs(m + 1)
        for i in range(group):
            to_x(m * group + i)
        if m + 1 < products:
            ours(m + 1)
    for load in loads[2:]:
        load.wait()
    order = []
    for k in range(chunks):
        order += [
            (k, 0, to_z, k), (k + 2, 1, to_y, k), (k + 3, 2, update, k), (k + 5, 3, column_in, k)
        ]
        late = k + 7
        order += [(late, 4, pieces_in, k), (late + 4, 5, from_y, k), (late + 4 + 1, 6, finish, k)]
    for _, _, stage, k in sorted(order, key=lambda entry: (entry[0], entry[1], entry[3])):
        stage(k)
    for k in range(chunks):
        drain(k)


def per_device(deep, wide, activations, cotangents, inner_params, inner_moment, outer_params, momentum):
    reps = lax.axis_size("rep")
    shards = lax.axis_size("shard")
    tokens, model = activations.shape
    kv = cotangents.shape[1]
    rows = outer_params.shape[0]
    width = 128
    chunks = kv // width
    bf16, f32 = jnp.bfloat16, jnp.float32
    tile = (rows, width)
    vmem = pl.BlockSpec(memory_space=pltpu.VMEM)
    dma = pltpu.SemaphoreType.DMA
    pieces = deep + wide - 1
    new_params, new_momentum, copied = pl.pallas_call(
        functools.partial(kernel, reps, deep, wide, chunks, tokens * shards),
        out_shape=(
            pltpu.VMEM((rows, kv), f32),
            pltpu.VMEM((rows, kv), f32),
            pltpu.VMEM((deep, wide, CORES, rows, kv), bf16),
        ),
        in_specs=[pl.BlockSpec(memory_space=pl.ANY)] * 6,
        out_specs=(vmem, vmem, vmem),
        scratch_shapes=[
            pltpu.VMEM((tokens, model), bf16),
            pltpu.VMEM((tokens, kv), bf16),
            pltpu.VMEM((1,) + (rows, kv), f32),
            pltpu.VMEM((1,) + (rows, kv), f32),
            pltpu.VMEM((rows, kv), f32),
            pltpu.VMEM((rows, kv), f32),
            pltpu.VMEM((deep * wide, CORES, rows, tokens), bf16),
            pltpu.VMEM((chunks, deep, wide) + tile, f32),
            pltpu.VMEM((chunks, deep, wide) + tile, bf16),
            pltpu.VMEM((chunks, deep, wide) + tile, bf16),
            pltpu.VMEM((chunks, wide - 1, deep) + tile, bf16),
            pltpu.VMEM((chunks, wide - 1, deep) + tile, bf16),
            pltpu.VMEM((chunks, deep - 1) + tile, bf16),
            pltpu.VMEM((chunks, deep - 1) + tile, bf16),
            pltpu.VMEM((chunks, reps) + tile, f32),
            pltpu.VMEM((chunks, deep, wide, CORES) + tile, bf16),
            dma((chunks,)), dma((chunks,)),
            dma((chunks, wide - 1)), dma((chunks, wide - 1)),
            dma((chunks, deep - 1)), dma((chunks, deep - 1)),
            dma((chunks, reps - 1)), dma((chunks, reps - 1)),
            dma((chunks, deep - 1)), dma((chunks, deep - 1)),
            dma((chunks, wide - 1)), dma((chunks, wide - 1)),
            dma((chunks, pieces, reps - 1)), dma((chunks, pieces, reps - 1)),
            dma((chunks, pieces)), dma((chunks, pieces)),
            dma((6,)),
        ],
        compiler_params=pltpu.CompilerParams(
            collective_id=0, has_side_effects=True, vmem_limit_bytes=61_000_000
        ),
    )(activations, cotangents, inner_params, inner_moment, outer_params, momentum)
    return (new_params, new_momentum, copied.reshape(model, kv))


def layout(mesh):
    chips = mesh.shape["shard"] // CORES
    first = mesh.devices.reshape(mesh.shape["rep"], mesh.shape["shard"])[0]
    wide = len({d.coords[0] for d in first}) if hasattr(first[0], "coords") else 2
    return chips // wide, wide


def solution(mesh):
    deep, wide = layout(mesh)
    in_specs = (
        P(("rep", "shard"), None),
        P(("rep", "shard"), None),
        P("rep", "shard", None),
        P("rep", "shard", None),
        P("shard", None),
        P("shard", None),
    )
    out_specs = (P("shard", None), P("shard", None), P())
    return jax.shard_map(
        functools.partial(per_device, deep, wide),
        mesh=mesh, in_specs=in_specs, out_specs=out_specs, check_vma=False,
    )
```
